32 devices in a mesh: rep: 2 (over y), shard: 16 (over z, x, core).
Axes of the slice: x: 2, y: 2, z: 4, core: 2. Of those that a mesh axis runs over, the one named last changes fastest.
Arguments:
- activations: bfloat16 [32768, 2048], P(('rep', 'shard')), may hold values from -6 to 6
- cotangents: bfloat16 [32768, 1024], P(('rep', 'shard')), may hold values from -768 to 768
- inner_params: float32 [2, 2048, 1024], P('rep', 'shard'), may hold values from -6 to 6
- inner_moment: float32 [2, 2048, 1024], P('rep', 'shard'), may hold values from 0.25 to 4
- outer_params: float32 [2048, 1024], P('shard'), may hold values from -6 to 6
- momentum: float32 [2048, 1024], P('shard'), may hold values from -3 to 3
Outputs:
- new_params: float32 [2048, 1024], P('shard')
- new_momentum: float32 [2048, 1024], P('shard')
- compute_copy: bfloat16 [2048, 1024], replicated
The draws below stay inside these ranges and needn't reach their ends.
All inputs are finite; a program needn't handle non-finite values.
Results may differ from the reference program's by a relative error of at most 0.007.
Values may be sent and summed in bfloat16 or wider, within the bound.
No kernel may reach another device: no remote copies, remote signals or barrier semaphores. Data moves between devices by JAX's collectives and lax.ppermute only.
A program may use at most 64 MiB of HBM per device.

```python
import math
import jax
import jax.numpy as jnp
from jax import lax

D = 2048
KV = 1024
TOK_DEV = 1024
REPS = 2
GROUP_TOK = 16384
TOKENS = 32768
N_SHARD = 16


def with_spikes(drawn, own_key, source, target, blocks, factor):
    def block_of(axis_at):
        return (jnp.arange(drawn.shape[axis_at]) // (drawn.shape[axis_at] // blocks)).reshape((-1,) + (1,) * (drawn.ndim - 1 - axis_at))

    first = jax.random.permutation(own_key, blocks)[block_of(target)]
    other_side = (block_of(target) + blocks // 2) % blocks
    return jnp.where((block_of(source) == first) | (block_of(source) == other_side), factor * drawn, drawn)


def shard_levels(stream_key, extent, pieces, least, top_value):
    gain, own = 1.0, jax.random.fold_in(stream_key, 6)
    for position, blocks in pieces:
        heights = jnp.exp(jax.random.uniform(jax.random.fold_in(own, position), (blocks,), jnp.float32, least / len(pieces), top_value / len(pieces)))
        gain = gain * jnp.repeat(heights, extent[position] // blocks).reshape([-1 if axis == position else 1 for axis in range(len(extent))])
    return gain


def bell_draw(stream_key, dims, width, bound, cuts=(), held_as=jnp.bfloat16):
    result = jax.random.normal(stream_key, dims, jnp.float32) * width
    if len(cuts) > 0:
        result = shard_levels(stream_key, dims, cuts, -0.22, 0.18) * result
    return jnp.clip(result, min=-bound, max=bound).astype(held_as)


def noise_with(own_key, dims, spread, reach, pieces, heavy, held_as=jnp.bfloat16):
    array = spread * jax.random.normal(own_key, dims, jnp.float32)
    if pieces:
        array = array * shard_levels(own_key, dims, pieces, -0.22, 0.18)
    return jnp.clip(with_spikes(array, jax.random.fold_in(own_key, 3), *heavy), -reach, reach).astype(held_as)


def setup_inputs(seed: int = 0) -> dict:
    seeds = jax.random.split(jax.random.key(seed), 7)
    activations = noise_with(seeds[0], (TOKENS, D), 1.0, 6.0, ((0, 32),), (0, 1, 32, 2.75))
    cotangents = bell_draw(seeds[1], (TOKENS, KV), (GROUP_TOK ** 0.5), 768.0, ((0, 32),))
    inner_params = bell_draw(seeds[2], (REPS, D, KV), 1.0, 6.0, ((0, 2), (1, 16)), jnp.float32)
    inner_moment = jnp.clip(jnp.exp(math.log(4.0) - 2.7725887 * jax.random.uniform(seeds[3], (REPS, D, KV), jnp.float32) ** shard_levels(seeds[3], (REPS, D, KV), ((0, 2), (1, 16)), -0.2, 0.2)), 0.25, 4.0)
    outer_params = bell_draw(seeds[4], (D, KV), 1.0, 6.0, ((0, 16),), jnp.float32)
    momentum = bell_draw(seeds[5], (D, KV), 0.5, 3.0, ((0, 16),), jnp.float32)
    return dict(activations=activations, cotangents=cotangents, inner_params=inner_params, inner_moment=inner_moment, outer_params=outer_params, momentum=momentum)


outer_rate = 0.7
inertia = 0.9
inner_rate = 0.3
epsilon = 1e-08

def reference(activations, cotangents, inner_params, inner_moment, outer_params, momentum):
    group_tok = TOK_DEV * N_SHARD
    delta_total = jnp.zeros(outer_params.shape, jnp.float32)
    for replica in range(REPS):
        rows_act = activations[replica * group_tok:(replica + 1) * group_tok]
        rows_cot = cotangents[replica * group_tok:(replica + 1) * group_tok]
        summed = lax.dot_general(rows_act, rows_cot, (((0,), (0,)), ((), ())), preferred_element_type=jnp.float32)
        mean_grad = summed / group_tok
        replica_params = inner_params[replica] - inner_rate * mean_grad / (jnp.sqrt(inner_moment[replica]) + epsilon)
        delta_total = delta_total + (outer_params - replica_params)
    pseudo_grad = delta_total / REPS
    new_momentum = inertia * momentum + pseudo_grad
    new_params = outer_params - outer_rate * (pseudo_grad + inertia * new_momentum)
    return (new_params, new_momentum, new_params.astype(jnp.bfloat16))
```

```python
import jax
import jax.numpy as jnp
from jax import lax
from jax.sharding import PartitionSpec as P

outer_rate = 0.7
inertia = 0.9
inner_rate = 0.3
epsilon = 1e-08


def outer_step(pseudo_grad, outer_rows, moment_rows):
    fresh_moment = inertia * moment_rows + pseudo_grad
    fresh_params = outer_rows - outer_rate * (pseudo_grad + inertia * fresh_moment)
    return (fresh_params, fresh_moment)


def flip(x, axis, bit):
    size = lax.axis_size(axis)
    return lax.ppermute(x, axis, [(i, i ^ (1 << bit)) for i in range(size)])


def half(x, dim, which):
    return lax.dynamic_index_in_dim(x, which, dim, keepdims=False)


def halving(part, dims, order, index):
    kept, got, dims = part, None, list(dims)
    for bit in order:
        at = dims.index(bit)
        mine = (index >> bit) & 1

        def piece(which):
            own = half(kept, at, which)
            if got is None:
                return own
            return (own.astype(jnp.float32) + half(got, at, which).astype(jnp.float32)).astype(jnp.bfloat16)

        sent = piece(1 - mine)
        arrived = flip(sent, "shard", bit)
        kept, got = piece(mine), arrived
        dims.remove(bit)
    return kept.astype(jnp.float32) + got.astype(jnp.float32)


def doubling(block, order, index):
    dims = []
    for bit in order:
        other = flip(block, "shard", bit)
        mine = (index >> bit) & 1
        at = sum(1 for b in dims if b > bit)
        low = jnp.where(mine == 0, block, other)
        high = jnp.where(mine == 0, other, block)
        block = jnp.stack([low, high], axis=at)
        dims.insert(at, bit)
    return block


def per_device(activations, cotangents, inner_params, inner_moment, outer_params, momentum):
    shard_count = lax.axis_size("shard")
    group_count = lax.axis_size("rep")
    index = lax.axis_index("shard")
    bits = shard_count.bit_length() - 1
    group_bits = group_count.bit_length() - 1
    group_tok = activations.shape[0] * shard_count
    rows, cols = outer_params.shape
    dims = list(range(bits - 1, -1, -1))
    summed = lax.dot_general(
        activations, cotangents, (((0,), (0,)), ((), ())), preferred_element_type=jnp.float32
    ).astype(jnp.bfloat16)
    blocks = summed.reshape((2,) * bits + (rows, cols))
    chip = list(range(1, bits))
    orders = [chip, chip[1:] + chip[:1]]
    width = cols // len(orders)
    new_params, new_momentum, copies = [], [], []
    for k, order in enumerate(orders):
        at = slice(k * width, (k + 1) * width)
        total = halving(blocks[..., at], dims, [0] + order, index)
        mean_grad = total / group_tok
        replica_params = inner_params[0, :, at] - inner_rate * mean_grad / (
            jnp.sqrt(inner_moment[0, :, at]) + epsilon
        )
        delta = outer_params[:, at] - replica_params
        for bit in range(group_bits):
            sent = delta.astype(jnp.bfloat16)
            delta = sent.astype(jnp.float32) + flip(sent, "rep", bit).astype(jnp.float32)
        params, moment = outer_step(delta / group_count, outer_params[:, at], momentum[:, at])
        new_params.append(params)
        new_momentum.append(moment)
        copies.append(doubling(params.astype(jnp.bfloat16), order[::-1] + [0], index))
    compute_copy = jnp.concatenate(copies, axis=-1).reshape(shard_count * rows, cols)
    return (
        jnp.concatenate(new_params, axis=-1),
        jnp.concatenate(new_momentum, axis=-1),
        compute_copy,
    )


def solution(mesh):
    in_specs = (
        P(("rep", "shard"), None),
        P(("rep", "shard"), None),
        P("rep", "shard", None),
        P("rep", "shard", None),
        P("shard", None),
        P("shard", None),
    )
    out_specs = (P("shard", None), P("shard", None), P())
    return jax.shard_map(
        per_device, mesh=mesh, in_specs=in_specs, out_specs=out_specs, check_vma=False
    )
```

```python
import jax
import jax.numpy as jnp
from jax import lax
from jax.experimental import pallas as pl
from jax.experimental.pallas import tpu as pltpu
from jax.sharding import PartitionSpec as P

outer_rate = 0.7
inertia = 0.9
inner_rate = 0.3
epsilon = 1e-08


def outer_step(pseudo_grad, outer_rows, moment_rows):
    fresh_moment = inertia * moment_rows + pseudo_grad
    fresh_params = outer_rows - outer_rate * (pseudo_grad + inertia * fresh_moment)
    return (fresh_params, fresh_moment)


CHUNKS = 2


def flip(x, axis, bit):
    size = lax.axis_size(axis)
    return lax.ppermute(x, axis, [(i, i ^ (1 << bit)) for i in range(size)])


def half(x, dim, which):
    return lax.dynamic_index_in_dim(x, which, dim, keepdims=False)


def summed_piece(kept, got, at, which):
    own = half(kept, at, which)
    if got is None:
        return own
    return (own.astype(jnp.float32) + half(got, at, which).astype(jnp.float32)).astype(jnp.bfloat16)


def halving(part, order, index):
    kept, got, dims = part, None, list(range(part.ndim - 3, -1, -1))
    for bit in order:
        at = dims.index(bit)
        mine = (index >> bit) & 1
        arrived = flip(summed_piece(kept, got, at, 1 - mine), "shard", bit)
        kept, got = summed_piece(kept, got, at, mine), arrived
        dims.remove(bit)
    return kept, got


def doubling(held, offsets, order):
    for bit in order[:-1]:
        held = jnp.concatenate([held, flip(held, "shard", bit)])
        offsets = offsets + [o ^ (1 << bit) for o in offsets]
    last = flip(held, "shard", order[-1])
    last_offsets = [o ^ (1 << order[-1]) for o in offsets]
    early = [(held, offsets), (flip(held, "shard", 0), [o ^ 1 for o in offsets])]
    late = [(last, last_offsets), (flip(last, "shard", 0), [o ^ 1 for o in last_offsets])]
    return early + late


def assemble(pieces, plain, index, rows, shape):
    flat = [x for group in plain for x in group]
    count = sum(len(p[1]) for p in pieces) + len(flat)

    def body(index_ref, *refs):
        sem = refs[-1]
        outs = refs[-2 - len(plain) : -1]
        copies = []

        def add(source, target):
            copies.append(pltpu.make_async_copy(source, target, sem.at[len(copies)]))

        for ref, (array, offsets, row, column) in zip(refs[: len(pieces)], pieces):
            for k, offset in enumerate(offsets):
                first = pl.multiple_of((index_ref[0] ^ offset) * rows + row, array.shape[1])
                add(ref.at[k], outs[0].at[pl.ds(first, array.shape[1]), pl.ds(column, array.shape[2])])
        at = len(pieces)
        for out, group in zip(outs[1:], plain):
            first = 0
            for x in group:
                add(refs[at], out.at[pl.ds(first, x.shape[0])])
                first, at = first + x.shape[0], at + 1
        for copy in copies:
            copy.start()
        for copy in copies:
            copy.wait()

    operands = [index.reshape(1)] + [p[0] for p in pieces] + flat
    in_specs = [pl.BlockSpec(memory_space=pltpu.SMEM)] + [pl.BlockSpec(memory_space=pltpu.VMEM)] * (len(operands) - 1)
    out_shape = [jax.ShapeDtypeStruct(shape, jnp.bfloat16)] + [
        jax.ShapeDtypeStruct((sum(x.shape[0] for x in group), group[0].shape[1]), group[0].dtype) for group in plain
    ]
    return pl.pallas_call(
        body,
        out_shape=out_shape,
        in_specs=in_specs,
        out_specs=[pl.BlockSpec(memory_space=pl.ANY)] * len(out_shape),
        scratch_shapes=[pltpu.SemaphoreType.DMA((count,))],
        name="assemble",
    )(*operands)


def per_device(activations, cotangents, inner_params, inner_moment, outer_params, momentum):
    shard_count = lax.axis_size("shard")
    group_count = lax.axis_size("rep")
    index = lax.axis_index("shard")
    bits = shard_count.bit_length() - 1
    group_tok = activations.shape[0] * shard_count
    rows, cols = outer_params.shape
    chip = list(range(1, bits - 1))
    orders = [chip, chip[1::-1] + chip[2:]]
    top = bits - 1
    width = cols // len(orders)
    parts = [
        lax.dot_general(
            activations,
            cotangents[:, k * width : (k + 1) * width],
            (((0,), (0,)), ((), ())),
            preferred_element_type=jnp.float32,
        )
        .astype(jnp.bfloat16)
        .reshape((2,) * bits + (rows, width))
        for k in range(len(orders))
    ]
    high = rows // CHUNKS
    new_params, new_momentum, pieces = [], [], []
    for j in range(CHUNKS):
        at = slice(j * high, (j + 1) * high)
        mine = (index >> top) & 1
        sums = [halving(part[..., at, :], [0] + order, index) for part, order in zip(parts, orders)]
        sent = [summed_piece(kept, got, 0, 1 - mine) for kept, got in sums]
        arrived = flip(jnp.concatenate(sent, axis=-1), "shard", top)
        own = jnp.concatenate([summed_piece(kept, got, 0, mine) for kept, got in sums], axis=-1)
        mean_grad = (own.astype(jnp.float32) + arrived.astype(jnp.float32)) / group_tok
        replica_params = inner_params[0, at] - inner_rate * mean_grad / (jnp.sqrt(inner_moment[0, at]) + epsilon)
        delta = outer_params[at] - replica_params
        for bit in range(group_count.bit_length() - 1):
            rounded = delta.astype(jnp.bfloat16)
            delta = rounded.astype(jnp.float32) + flip(rounded, "rep", bit).astype(jnp.float32)
        params, moment = outer_step(delta / group_count, outer_params[at], momentum[at])
        new_params.append(params)
        new_momentum.append(moment)
        block = params.astype(jnp.bfloat16)
        pair = jnp.stack([block, flip(block, "shard", top)])
        for k, order in enumerate(orders):
            held = pair[..., k * width : (k + 1) * width]
            gathered = doubling(held, [0, 1 << top], order[::-1])
            pieces += [(x, o, j * high, k * width) for x, o in gathered]
    shape = (shard_count * rows, cols)
    compute_copy, params, moments = assemble(pieces, [new_params, new_momentum], index, rows, shape)
    return (params, moments, compute_copy)


def solution(mesh):
    in_specs = (
        P(("rep", "shard"), None),
        P(("rep", "shard"), None),
        P("rep", "shard", None),
        P("rep", "shard", None),
        P("shard", None),
        P("shard", None),
    )
    out_specs = (P("shard", None), P("shard", None), P())
    return jax.shard_map(
        per_device, mesh=mesh, in_specs=in_specs, out_specs=out_specs, check_vma=False
    )
```
